32 devices in a mesh: comp: 8 (over z, core), blk: 4 (over y, x).
Axes of the slice: x: 2, y: 2, z: 4, core: 2. Of those that a mesh axis runs over, the one named last changes fastest.
Arguments:
- state_now: float32 [8, 6, 32, 32, 256], P('comp', None, 'blk'), may hold values from -5 to 5
- state_prev: float32 [8, 6, 32, 32, 256], P('comp', None, 'blk'), may hold values from -5 to 5
- viscosity: float32 [8, 32, 32, 256], P('comp', 'blk'), may hold values from 0.05 to 0.5
- jacobian: float32 [8, 3, 6, 6], P('comp'), may hold values from -0.4 to 0.4
- donor_cell: int32 [8, 4, 8, 2, 8, 128], P('comp', 'blk'), may hold values from 0 to 57343, as said below
- interp_weight: float32 [8, 4, 8, 2, 8, 128], P('comp', 'blk'), may hold values from 0 to 1
- recv_cell: int32 [8, 4, 8, 2, 128], P('comp', 'blk'), may hold values from 0 to 57343, as said below
- pair_tiles: int32 [4, 8, 8], P('blk'), may hold values from 0 to 2, as said below
Outputs:
- state_next: float32 [8, 6, 32, 32, 256], P('comp', None, 'blk')
The draws below stay inside these ranges and needn't reach their ends.
Inputs may be any that keep to these rules, and one draw needn't show every extreme that they name: `donor_cell`: the cells of one donor tile point are the eight corners of a cube of adjacent cells, corner k = 4 i + 2 j + l offset by (i, j, l). `recv_cell`: the receiving cells of one device are all different. `pair_tiles`: for each block index some destination component takes 2 tiles from every source component.
All inputs are finite; a program needn't handle non-finite values.
Results may differ from the reference program's by a relative error of at most 0.0003.
Values sent between devices are 32-bit elements; how exact they have to be, the bound alone decides.
A program may use at most 128 MiB of HBM per device.

```python
import math
import jax
import jax.numpy as jnp
from jax import lax

NV = 6
CX = 8
CY = 32
CZ = 256
SLOT = 2
TILE = 128
SUBITERS = 2
COMPS = 8
BLKS = 4
NX = 32
CELLS = 65536


def draw_donor_cell(key, part):
    shape = (COMPS, BLKS, COMPS, SLOT, TILE)
    first = jax.random.randint(jax.random.fold_in(key, 11), shape, 0, CX - 2)
    second = jax.random.randint(jax.random.fold_in(key, 12), shape, 0, CY - 1)
    third = jax.random.randint(jax.random.fold_in(key, 13), shape, 0, CZ - 1)
    corners = []
    for corner in range(8):
        off_a = corner // 4
        off_b = corner // 2 % 2
        off_c = corner % 2
        corners.append(((first + off_a) * CY + (second + off_b)) * CZ + (third + off_c))
    return jnp.stack(corners, axis=4).astype(jnp.int32)


def draw_interp_weight(key, part):
    shape = (3, COMPS, BLKS, COMPS, SLOT, TILE)
    frac = jax.random.uniform(jax.random.fold_in(key, 22), shape, jnp.float32)
    corners = []
    for corner in range(8):
        off_a = corner // 4
        off_b = corner // 2 % 2
        off_c = corner % 2
        part_a = frac[0] if off_a == 1 else 1.0 - frac[0]
        part_b = frac[1] if off_b == 1 else 1.0 - frac[1]
        part_c = frac[2] if off_c == 1 else 1.0 - frac[2]
        corners.append(part_a * part_b * part_c)
    return jnp.stack(corners, axis=4).astype(jnp.float32)


def draw_recv_cell(key, part):
    keys = jax.random.split(jax.random.fold_in(key, 31), COMPS * BLKS)

    def one_device(single):
        return jax.random.permutation(single, (CX - 1) * CY * CZ)[:COMPS * SLOT * TILE]
    chosen = jax.vmap(one_device)(keys)
    return chosen.reshape(COMPS, BLKS, COMPS, SLOT, TILE).astype(jnp.int32)


def draw_pair_tiles(key, part):
    counts = jax.random.randint(jax.random.fold_in(key, 41), (BLKS, COMPS, COMPS), 0, SLOT + 1)
    column = jax.random.randint(jax.random.fold_in(key, 42), (BLKS,), 0, COMPS)
    full = jnp.arange(COMPS, dtype=jnp.int32)[None, None, :] == column[:, None, None]
    return jnp.where(full, SLOT, counts).astype(jnp.int32)


def block_scale(own_key, extent, cuts, smallest, high):
    gain = 1.0
    for axis_at, shards_of in cuts:
        heights = jax.random.uniform(jax.random.fold_in(jax.random.fold_in(own_key, 6), axis_at), (shards_of,), jnp.float32, smallest / len(cuts), high / len(cuts))
        gain = gain * jnp.repeat(jnp.exp(heights), extent[axis_at] // shards_of).reshape((-1,) + (1,) * (len(extent) - 1 - axis_at))
    return gain


def bell_draw(own_key, shape, deviation, limit, pieces=(), held_as=jnp.bfloat16):
    factor_of = block_scale(own_key, shape, pieces, -0.22, 0.18) if pieces else 1.0
    drawn = jax.random.normal(own_key, shape, jnp.float32) * deviation * factor_of
    return jnp.minimum(jnp.maximum(drawn, -limit), limit).astype(held_as)


def setup_inputs(seed: int = 0) -> dict:
    streams_of = jax.random.split(jax.random.key(seed), 9)
    return {
        "state_now": bell_draw(streams_of[0], (COMPS, NV, NX, CY, CZ), 1.0, 5.0, ((0, 8), (2, 4)), jnp.float32),
        "state_prev": bell_draw(streams_of[1], (COMPS, NV, NX, CY, CZ), 1.0, 5.0, ((0, 8), (2, 4)), jnp.float32),
        "viscosity": jnp.clip(jnp.exp(math.log(0.5) - 2.3025851 * jax.random.uniform(streams_of[2], (COMPS, NX, CY, CZ), jnp.float32) ** block_scale(streams_of[2], (COMPS, NX, CY, CZ), ((0, 8), (1, 4)), -0.2, 0.2)), 0.05, 0.5),
        "jacobian": bell_draw(streams_of[3], (COMPS, 3, NV, NV), 0.1, 0.4, ((0, 8),), jnp.float32),
        "donor_cell": draw_donor_cell(jax.random.fold_in(streams_of[8], 71), 0),
        "interp_weight": draw_interp_weight(jax.random.fold_in(streams_of[8], 71), 0),
        "recv_cell": draw_recv_cell(jax.random.fold_in(streams_of[8], 71), 0),
        "pair_tiles": draw_pair_tiles(jax.random.fold_in(streams_of[8], 71), 0),
    }


time_scale = 0.5
pseudo_diag = 2.5


def mix(jac_dim, field):
    return jnp.einsum('vw,wxyz->vxyz', jac_dim, field, precision=lax.Precision.HIGHEST)


def flux(padded, kappa, jac):
    centre = padded[:, 1:-1]
    along_x = (padded[:, 2:] - padded[:, :-2]) * 0.5
    spread = jnp.pad(centre, ((0, 0), (0, 0), (1, 1), (1, 1)))
    along_y = (spread[:, :, 2:, 1:-1] - spread[:, :, :-2, 1:-1]) * 0.5
    along_z = (spread[:, :, 1:-1, 2:] - spread[:, :, 1:-1, :-2]) * 0.5
    beside = padded[:, 2:] + padded[:, :-2] + spread[:, :, 2:, 1:-1] + spread[:, :, :-2, 1:-1]
    beside = beside + spread[:, :, 1:-1, 2:] + spread[:, :, 1:-1, :-2]
    convect = mix(jac[0], along_x) + mix(jac[1], along_y) + mix(jac[2], along_z)
    return convect + kappa * (6.0 * centre - beside)


def relax(rstar, padded_step, kappa, diag, jac):
    centre = padded_step[:, 1:-1]
    return -(rstar + flux(padded_step, kappa, jac) - 6.0 * kappa * centre) / diag


def pad_rows(field):
    return jnp.pad(field, ((0, 0), (1, 1), (0, 0), (0, 0)))


def subiteration(items):
    state, now, prev, kappa, jac = items
    diag = pseudo_diag + 6.0 * kappa
    rstar = time_scale * (3.0 * state - 4.0 * now + prev) + flux(pad_rows(state), kappa, jac)
    first = -rstar / diag
    second = relax(rstar, pad_rows(first), kappa, diag, jac)
    third = relax(rstar, pad_rows(second), kappa, diag, jac)
    return state + third


def fringe(state, donor_cell, interp_weight, recv_cell, pair_tiles):
    comps = state.shape[0]
    nvar = state.shape[1]
    flat = state.reshape(comps, nvar, BLKS, CELLS).transpose(2, 0, 1, 3)
    donors = donor_cell.transpose(1, 0, 2, 3, 4, 5)
    weights = interp_weight.transpose(1, 0, 2, 3, 4, 5)
    cells_all = recv_cell.transpose(1, 0, 2, 3, 4)

    def one_block(items):
        blocks, donor_b, weight_b, cell_b, live_b = items

        def pick(block, index):
            return block[:, index.reshape(-1)]

        values = jax.vmap(pick)(blocks, donor_b).reshape(comps, nvar, comps, SLOT, 8, TILE)
        interp = jnp.einsum('caskp,avcskp->cvasp', weight_b, values, precision=lax.Precision.HIGHEST)

        def place(block, cells, incoming, live):
            index = cells.reshape(-1)
            keep = jnp.arange(SLOT, dtype=jnp.int32)[None, :] < live[:, None]
            keep = jnp.broadcast_to(keep[:, :, None], (comps, SLOT, TILE)).reshape(-1)
            old = block[:, index]
            return block.at[:, index].set(jnp.where(keep[None, :], incoming.reshape(nvar, -1), old))

        return jax.vmap(place)(blocks, cell_b, interp, live_b.T)

    result = lax.map(one_block, (flat, donors, weights, cells_all, pair_tiles))
    return result.transpose(1, 2, 0, 3).reshape(state.shape)


def reference(state_now, state_prev, viscosity, jacobian, donor_cell, interp_weight, recv_cell, pair_tiles):
    state = state_now
    for sub in range(SUBITERS):
        state = lax.map(subiteration, (state, state_now, state_prev, viscosity, jacobian))
        state = fringe(state, donor_cell, interp_weight, recv_cell, pair_tiles)
    return state
```

```python
import functools

import jax
import jax.numpy as jnp
from jax import lax
from jax.experimental import pallas as pl
from jax.experimental.pallas import tpu as pltpu
from jax.sharding import PartitionSpec as P

SUBITERS = 2


time_scale = 0.5
pseudo_diag = 2.5

MESH = pl.DeviceIdType.MESH
VMEM_LIMIT = 60 * 1024 * 1024
F32 = jnp.float32
BF16 = jnp.bfloat16


def split(value):
    high = value.astype(BF16)
    low = (value - high.astype(F32)).astype(BF16)
    return high, low


def fill_mix(jac_ref, mix_hi, mix_lo, nvar, width_y):
    columns = mix_hi.shape[1]
    row = lax.broadcasted_iota(jnp.int32, (width_y, columns), 0)
    col = lax.broadcasted_iota(jnp.int32, (width_y, columns), 1)
    for v in range(nvar):
        block = jnp.zeros((width_y, columns), F32)
        for d in range(3):
            for w in range(nvar):
                block = jnp.where(col == row + (d * nvar + w) * width_y, 0.5 * jac_ref[d, v, w], block)
        high, low = split(block)
        mix_hi[v * width_y : (v + 1) * width_y, :] = high
        mix_lo[v * width_y : (v + 1) * width_y, :] = low


def flux_plane(centre, below, above, kappa, mix_hi, mix_lo):
    shape = centre.shape
    nvar, width_y, width_z = shape
    flat = centre.reshape(nvar * width_y, width_z)
    at_y = lax.broadcasted_iota(jnp.int32, shape, 1)
    at_z = lax.broadcasted_iota(jnp.int32, shape, 2)

    def moved(shift, axis, keep):
        return jnp.where(keep, pltpu.roll(flat, shift, axis).reshape(shape), 0.0)

    next_y = moved(nvar * width_y - 1, 0, at_y < width_y - 1)
    last_y = moved(1, 0, at_y > 0)
    next_z = moved(width_z - 1, 1, at_z < width_z - 1)
    last_z = moved(1, 1, at_z > 0)
    beside = (above + below) + (next_y + last_y) + (next_z + last_z)
    diffs = [above - below, next_y - last_y, next_z - last_z]
    diffs = jnp.concatenate([d.reshape(flat.shape) for d in diffs], axis=0)
    high, low = split(diffs)
    hi = mix_hi[...]
    convect = jnp.dot(hi, high, preferred_element_type=F32)
    convect += jnp.dot(mix_lo[...], high, preferred_element_type=F32)
    convect += jnp.dot(hi, low, preferred_element_type=F32)
    return convect.reshape(shape) + kappa[None] * (6.0 * centre - beside)


def relax_kernel(
    count, jac_ref, state_ref, now_ref, prev_ref, kappa_ref, out_ref,
    halo, rstar, first, second, mix_hi, mix_lo, send_sem, recv_sem,
):
    me = lax.axis_index("blk")
    right = lax.rem(me + 1, count)
    left = lax.rem(me + count - 1, count)
    has_left = me > 0
    has_right = me < count - 1
    nvar, rows, width_y, width_z = state_ref.shape
    barrier = pltpu.get_barrier_semaphore()

    @pl.when(has_left)
    def _():
        pl.semaphore_signal(barrier, inc=1, device_id={"blk": left}, device_id_type=MESH)

    @pl.when(has_right)
    def _():
        pl.semaphore_signal(barrier, inc=1, device_id={"blk": right}, device_id_type=MESH)

    @pl.when(jnp.logical_not(has_left))
    def _():
        for k in range(3):
            halo[k, 0] = jnp.zeros((nvar, width_y, width_z), F32)

    @pl.when(jnp.logical_not(has_right))
    def _():
        for k in range(3):
            halo[k, 1] = jnp.zeros((nvar, width_y, width_z), F32)

    pl.semaphore_wait(barrier, has_left.astype(jnp.int32) + has_right.astype(jnp.int32))

    fields = [state_ref, first, second]

    def to_left(k):
        return pltpu.make_async_remote_copy(
            src_ref=fields[k].at[:, 0], dst_ref=halo.at[k, 1],
            send_sem=send_sem.at[k, 1], recv_sem=recv_sem.at[k, 1],
            device_id={"blk": left}, device_id_type=MESH,
        )

    def to_right(k):
        return pltpu.make_async_remote_copy(
            src_ref=fields[k].at[:, rows - 1], dst_ref=halo.at[k, 0],
            send_sem=send_sem.at[k, 0], recv_sem=recv_sem.at[k, 0],
            device_id={"blk": right}, device_id_type=MESH,
        )

    def start(k):
        @pl.when(has_left)
        def _():
            to_left(k).start()

        @pl.when(has_right)
        def _():
            to_right(k).start()

    def arrive(k):
        @pl.when(has_left)
        def _():
            to_right(k).wait_recv()

        @pl.when(has_right)
        def _():
            to_left(k).wait_recv()

    def plane(k, x, below, above):
        kappa = kappa_ref[x]
        centre = fields[k][:, x]
        flow = flux_plane(centre, below, above, kappa, mix_hi, mix_lo)
        scale = -1.0 / (pseudo_diag + 6.0 * kappa)
        if k == 0:
            base = time_scale * (3.0 * centre - 4.0 * now_ref[:, x] + prev_ref[:, x]) + flow
            rstar[:, x] = base
            first[:, x] = base * scale[None]
        else:
            step = (rstar[:, x] + flow - 6.0 * kappa[None] * centre) * scale[None]
            if k == 1:
                second[:, x] = step
            else:
                out_ref[:, x] = state_ref[:, x] + step

    start(0)
    fill_mix(jac_ref, mix_hi, mix_lo, nvar, width_y)
    for k in range(3):
        field = fields[k]

        def inner(x, carry, k=k, field=field):
            plane(k, x, field[:, x - 1], field[:, x + 1])
            return carry

        lax.fori_loop(1, rows - 1, inner, 0)
        arrive(k)
        plane(k, 0, halo[k, 0], field[:, 1])
        plane(k, rows - 1, field[:, rows - 2], halo[k, 1])
        if k < 2:
            start(k + 1)
    for k in range(3):
        @pl.when(has_left)
        def _(k=k):
            to_left(k).wait_send()

        @pl.when(has_right)
        def _(k=k):
            to_right(k).wait_send()


def relax(jac, state, now, prev, kappa):
    count = lax.axis_size("blk")
    nvar, rows, width_y, width_z = state.shape
    vmem = pl.BlockSpec(memory_space=pltpu.VMEM)
    whole = pltpu.VMEM(state.shape, F32)
    mixed = pltpu.VMEM((nvar * width_y, 3 * nvar * width_y), BF16)
    return pl.pallas_call(
        functools.partial(relax_kernel, count),
        out_shape=jax.ShapeDtypeStruct(state.shape, F32),
        in_specs=[pl.BlockSpec(memory_space=pltpu.SMEM)] + [vmem] * 4,
        out_specs=vmem,
        scratch_shapes=[
            pltpu.VMEM((3, 2, nvar, width_y, width_z), F32),
            whole, whole, whole, mixed, mixed,
            pltpu.SemaphoreType.DMA((3, 2)),
            pltpu.SemaphoreType.DMA((3, 2)),
        ],
        compiler_params=pltpu.CompilerParams(
            collective_id=0, has_side_effects=True, vmem_limit_bytes=VMEM_LIMIT
        ),
        name="relax",
    )(jac, state, now, prev, kappa)


def gather_kernel(strides, live_ref, state_ref, base_ref, weight_ref, out_ref, packed):
    nvar, pairs, width_z = state_ref.shape
    width_y, shift = strides
    tiles, _, tile = base_ref.shape
    for v in range(nvar):
        high, low = split(state_ref[v])
        packed[v * pairs : (v + 1) * pairs, :width_z] = high
        packed[v * pairs : (v + 1) * pairs, width_z:] = low

    def one(t, carry):
        @pl.when(live_ref[t] > 0)
        def _():
            base = base_ref[t]
            pair = lax.shift_right_logical(base, shift)
            depth = jnp.bitwise_and(base, width_z - 1)
            depth = jnp.concatenate([depth, depth + 1], axis=1)
            pair = jnp.concatenate([pair, pair], axis=1)
            at_z = lax.broadcasted_iota(jnp.int32, (width_z, 2 * tile), 0)
            hot = jnp.where(at_z == depth, 1.0, 0.0).astype(BF16)
            hot = jnp.concatenate([hot, hot], axis=0)
            found = jnp.dot(packed[...], hot, preferred_element_type=F32)
            at_pair = lax.broadcasted_iota(jnp.int32, (pairs, 2 * tile), 0) - pair
            weights = weight_ref[t]
            spread = jnp.zeros((pairs, 2 * tile), F32)
            for i in range(2):
                for j in range(2):
                    k = 4 * i + 2 * j
                    row = jnp.concatenate([weights[k : k + 1], weights[k + 1 : k + 2]], axis=1)
                    spread = jnp.where(at_pair == i * width_y + j, row, spread)
            total = (found.reshape(nvar, pairs, 2 * tile) * spread[None]).sum(axis=1)
            out_ref[t] = total[:, :tile] + total[:, tile:]

        @pl.when(live_ref[t] <= 0)
        def _():
            out_ref[t] = jnp.zeros((nvar, tile), F32)

        return carry

    lax.fori_loop(0, tiles, one, 0)


def gather(live, state, base, weights):
    nvar, rows, width_y, width_z = state.shape
    pairs = rows * width_y
    tiles, _, tile = base.shape
    vmem = pl.BlockSpec(memory_space=pltpu.VMEM)
    return pl.pallas_call(
        functools.partial(gather_kernel, (width_y, width_z.bit_length() - 1)),
        out_shape=jax.ShapeDtypeStruct((tiles, nvar, tile), F32),
        in_specs=[pl.BlockSpec(memory_space=pltpu.SMEM)] + [vmem] * 3,
        out_specs=vmem,
        scratch_shapes=[pltpu.VMEM((nvar * pairs, 2 * width_z), BF16)],
        compiler_params=pltpu.CompilerParams(vmem_limit_bytes=VMEM_LIMIT),
        name="gather",
    )(live, state.reshape(nvar, pairs, width_z), base, weights)


def scatter_kernel(shift, state_ref, cell_ref, value_ref, out_ref, rows_ref, total):
    nvar, pairs, width_z = state_ref.shape
    tiles, _, tile = cell_ref.shape
    total[...] = jnp.zeros_like(total)
    rows_ref[nvar * pairs :, tile:] = jnp.zeros((pairs, tile), BF16)

    def one(t, carry):
        cell = cell_ref[t]
        pair = lax.shift_right_arithmetic(cell, shift)
        depth = jnp.bitwise_and(cell, width_z - 1)
        hot = lax.broadcasted_iota(jnp.int32, (width_z, tile), 0) == depth
        hot = jnp.where(hot, 1.0, 0.0).astype(BF16)
        hot = jnp.concatenate([hot, hot], axis=1)
        here = lax.broadcasted_iota(jnp.int32, (pairs, tile), 0) == pair
        values = value_ref[t]
        high = values.astype(BF16).astype(F32)
        low = values - high
        for v in range(nvar):
            at = slice(v * pairs, (v + 1) * pairs)
            rows_ref[at, :tile] = jnp.where(here, high[v : v + 1], 0.0).astype(BF16)
            rows_ref[at, tile:] = jnp.where(here, low[v : v + 1], 0.0).astype(BF16)
        rows_ref[nvar * pairs :, :tile] = jnp.where(here, 1.0, 0.0).astype(BF16)
        total[...] += lax.dot_general(
            rows_ref[...], hot, (((1,), (1,)), ((), ())), preferred_element_type=F32
        )
        return carry

    lax.fori_loop(0, tiles, one, 0)
    hit = total[nvar * pairs :, :] > 0.5
    for v in range(nvar):
        out_ref[v] = jnp.where(hit, total[v * pairs : (v + 1) * pairs, :], state_ref[v])


def scatter(state, cells, values):
    nvar, rows, width_y, width_z = state.shape
    pairs = rows * width_y
    tile = cells.shape[2]
    vmem = pl.BlockSpec(memory_space=pltpu.VMEM)
    out = pl.pallas_call(
        functools.partial(scatter_kernel, width_z.bit_length() - 1),
        out_shape=jax.ShapeDtypeStruct((nvar, pairs, width_z), F32),
        in_specs=[vmem] * 3,
        out_specs=vmem,
        scratch_shapes=[
            pltpu.VMEM(((nvar + 1) * pairs, 2 * tile), BF16),
            pltpu.VMEM(((nvar + 1) * pairs, width_z), F32),
        ],
        compiler_params=pltpu.CompilerParams(vmem_limit_bytes=VMEM_LIMIT),
        name="scatter",
    )(state.reshape(nvar, pairs, width_z), cells, values)
    return out.reshape(state.shape)


def shards(
    state_now, state_prev, viscosity, jacobian, donor_cell, interp_weight, recv_cell, pair_tiles
):
    now = state_now[0]
    prev = state_prev[0]
    kappa = viscosity[0]
    jac = jacobian[0]
    nvar = now.shape[0]
    comps = lax.axis_size("comp")
    mine = lax.axis_index("comp")
    slots, corners, tile = donor_cell.shape[3:]
    tiles = comps * slots
    slot = jnp.arange(slots, dtype=jnp.int32)[None, :]
    live_in = lax.dynamic_index_in_dim(pair_tiles[0], mine, 1, keepdims=False)
    live_out = lax.dynamic_index_in_dim(pair_tiles[0], mine, 0, keepdims=False)
    keep = (slot < live_in[:, None]).reshape(tiles, 1, 1)
    cells = jnp.where(keep, recv_cell[0, 0].reshape(tiles, 1, tile), -1)
    send = (slot < live_out[:, None]).astype(jnp.int32).reshape(tiles)
    base = donor_cell[0, 0].reshape(tiles, corners, tile)[:, :1]
    held = lax.all_to_all(interp_weight[0, 0], "comp", split_axis=0, concat_axis=0, tiled=True)
    held = held.reshape(tiles, corners, tile)
    state = now
    for sub in range(SUBITERS):
        state = relax(jac, state, now, prev, kappa)
        packed = gather(send, state, base, held)
        packed = packed.reshape(comps, slots * nvar, tile)
        arrived = lax.all_to_all(packed, "comp", split_axis=0, concat_axis=0, tiled=True)
        state = scatter(state, cells, arrived.reshape(tiles, nvar, tile))
    return state[None]


def solution(mesh):
    in_specs = (
        P("comp", None, "blk", None, None),
        P("comp", None, "blk", None, None),
        P("comp", "blk", None, None),
        P("comp", None, None, None),
        P("comp", "blk", None, None, None, None),
        P("comp", "blk", None, None, None, None),
        P("comp", "blk", None, None, None),
        P("blk", None, None),
    )
    out_specs = P("comp", None, "blk", None, None)
    return jax.shard_map(shards, mesh=mesh, in_specs=in_specs, out_specs=out_specs, check_vma=False)
```

```python
import functools

import jax
import jax.numpy as jnp
from jax import lax
from jax.experimental import pallas as pl
from jax.experimental.pallas import tpu as pltpu
from jax.sharding import PartitionSpec as P

SUBITERS = 2


time_scale = 0.5
pseudo_diag = 2.5

MESH = pl.DeviceIdType.MESH
VMEM_LIMIT = 60 * 1024 * 1024
F32 = jnp.float32
BF16 = jnp.bfloat16


def split(value):
    high = value.astype(BF16)
    low = (value - high.astype(F32)).astype(BF16)
    return high, low


def fill_mix(jac_ref, mix_hi, mix_lo, nvar, width_y):
    columns = mix_hi.shape[1]
    row = lax.broadcasted_iota(jnp.int32, (width_y, columns), 0)
    col = lax.broadcasted_iota(jnp.int32, (width_y, columns), 1)
    for v in range(nvar):
        block = jnp.zeros((width_y, columns), F32)
        for d in range(3):
            for w in range(nvar):
                block = jnp.where(col == row + (d * nvar + w) * width_y, 0.5 * jac_ref[d, v, w], block)
        high, low = split(block)
        mix_hi[v * width_y : (v + 1) * width_y, :] = high
        mix_lo[v * width_y : (v + 1) * width_y, :] = low


def flux_plane(centre, below, above, kappa, mix_hi, mix_lo):
    shape = centre.shape
    nvar, width_y, width_z = shape
    flat = centre.reshape(nvar * width_y, width_z)
    at_y = lax.broadcasted_iota(jnp.int32, shape, 1)
    at_z = lax.broadcasted_iota(jnp.int32, shape, 2)

    def moved(shift, axis, keep):
        return jnp.where(keep, pltpu.roll(flat, shift, axis).reshape(shape), 0.0)

    next_y = moved(nvar * width_y - 1, 0, at_y < width_y - 1)
    last_y = moved(1, 0, at_y > 0)
    next_z = moved(width_z - 1, 1, at_z < width_z - 1)
    last_z = moved(1, 1, at_z > 0)
    beside = (above + below) + (next_y + last_y) + (next_z + last_z)
    diffs = [above - below, next_y - last_y, next_z - last_z]
    diffs = jnp.concatenate([d.reshape(flat.shape) for d in diffs], axis=0)
    high, low = split(diffs)
    hi = mix_hi[...]
    convect = jnp.dot(hi, high, preferred_element_type=F32)
    convect += jnp.dot(mix_lo[...], high, preferred_element_type=F32)
    convect += jnp.dot(hi, low, preferred_element_type=F32)
    return convect.reshape(shape) + kappa[None] * (6.0 * centre - beside)


def comp_copies(comps, source_ref, landing, send_sem, recv_sem):
    mine = lax.axis_index("comp")

    def copy(d):
        peer = lax.rem(mine + d, comps)
        return pltpu.make_async_remote_copy(
            src_ref=source_ref.at[peer], dst_ref=landing.at[d],
            send_sem=send_sem.at[d], recv_sem=recv_sem.at[d],
            device_id={"comp": peer}, device_id_type=MESH,
        )

    return mine, copy


def greet_comps(comps, barrier):
    mine = lax.axis_index("comp")
    for d in range(1, comps):
        peer = lax.rem(mine + d, comps)
        pl.semaphore_signal(barrier, inc=1, device_id={"comp": peer}, device_id_type=MESH)


def relax_kernel(count, comps, jac_ref, state_ref, now_ref, prev_ref, kappa_ref, *refs):
    if comps:
        weight_ref, out_ref, held_ref = refs[:3]
        landing, weight_send, weight_recv = refs[-3:]
        refs = refs[3:-3]
    else:
        out_ref = refs[0]
        refs = refs[1:]
    halo, rstar, first, second, mix_hi, mix_lo, send_sem, recv_sem = refs
    me = lax.axis_index("blk")
    right = lax.rem(me + 1, count)
    left = lax.rem(me + count - 1, count)
    has_left = me > 0
    has_right = me < count - 1
    nvar, rows, width_y, width_z = state_ref.shape
    barrier = pltpu.get_barrier_semaphore()

    @pl.when(has_left)
    def _():
        pl.semaphore_signal(barrier, inc=1, device_id={"blk": left}, device_id_type=MESH)

    @pl.when(has_right)
    def _():
        pl.semaphore_signal(barrier, inc=1, device_id={"blk": right}, device_id_type=MESH)

    if comps:
        greet_comps(comps, barrier)

    @pl.when(jnp.logical_not(has_left))
    def _():
        for k in range(3):
            halo[k, 0] = jnp.zeros((nvar, width_y, width_z), F32)

    @pl.when(jnp.logical_not(has_right))
    def _():
        for k in range(3):
            halo[k, 1] = jnp.zeros((nvar, width_y, width_z), F32)

    peers = has_left.astype(jnp.int32) + has_right.astype(jnp.int32)
    pl.semaphore_wait(barrier, peers + max(comps - 1, 0))

    fields = [state_ref, first, second]

    def to_left(k):
        return pltpu.make_async_remote_copy(
            src_ref=fields[k].at[:, 0], dst_ref=halo.at[k, 1],
            send_sem=send_sem.at[k, 1], recv_sem=recv_sem.at[k, 1],
            device_id={"blk": left}, device_id_type=MESH,
        )

    def to_right(k):
        return pltpu.make_async_remote_copy(
            src_ref=fields[k].at[:, rows - 1], dst_ref=halo.at[k, 0],
            send_sem=send_sem.at[k, 0], recv_sem=recv_sem.at[k, 0],
            device_id={"blk": right}, device_id_type=MESH,
        )

    def start(k):
        @pl.when(has_left)
        def _():
            to_left(k).start()

        @pl.when(has_right)
        def _():
            to_right(k).start()

    def arrive(k):
        @pl.when(has_left)
        def _():
            to_right(k).wait_recv()

        @pl.when(has_right)
        def _():
            to_left(k).wait_recv()

    def plane(k, x, below, above):
        kappa = kappa_ref[x]
        centre = fields[k][:, x]
        flow = flux_plane(centre, below, above, kappa, mix_hi, mix_lo)
        scale = -1.0 / (pseudo_diag + 6.0 * kappa)
        if k == 0:
            base = time_scale * (3.0 * centre - 4.0 * now_ref[:, x] + prev_ref[:, x]) + flow
            rstar[:, x] = base
            first[:, x] = base * scale[None]
        else:
            step = (rstar[:, x] + flow - 6.0 * kappa[None] * centre) * scale[None]
            if k == 1:
                second[:, x] = step
            else:
                out_ref[:, x] = state_ref[:, x] + step

    start(0)
    if comps:
        mine, copy = comp_copies(comps, weight_ref, landing, weight_send, weight_recv)
        for d in range(1, comps):
            copy(d).start()
        held_ref[mine] = weight_ref[mine]
    fill_mix(jac_ref, mix_hi, mix_lo, nvar, width_y)
    for k in range(3):
        field = fields[k]

        def inner(x, carry, k=k, field=field):
            plane(k, x, field[:, x - 1], field[:, x + 1])
            return carry

        lax.fori_loop(1, rows - 1, inner, 0)
        arrive(k)
        plane(k, 0, halo[k, 0], field[:, 1])
        plane(k, rows - 1, field[:, rows - 2], halo[k, 1])
        if k < 2:
            start(k + 1)
    if comps:
        for d in range(1, comps):
            copy(d).wait()
            held_ref[lax.rem(mine - d + comps, comps)] = landing[d]
    for k in range(3):
        @pl.when(has_left)
        def _(k=k):
            to_left(k).wait_send()

        @pl.when(has_right)
        def _(k=k):
            to_right(k).wait_send()


def relax(jac, state, now, prev, kappa, weights=None):
    count = lax.axis_size("blk")
    nvar, rows, width_y, width_z = state.shape
    vmem = pl.BlockSpec(memory_space=pltpu.VMEM)
    whole = pltpu.VMEM(state.shape, F32)
    mixed = pltpu.VMEM((nvar * width_y, 3 * nvar * width_y), BF16)
    operands = [jac, state, now, prev, kappa]
    outs = [jax.ShapeDtypeStruct(state.shape, F32)]
    scratch = [
        pltpu.VMEM((3, 2, nvar, width_y, width_z), F32),
        whole, whole, whole, mixed, mixed,
        pltpu.SemaphoreType.DMA((3, 2)),
        pltpu.SemaphoreType.DMA((3, 2)),
    ]
    comps = 0
    if weights is not None:
        comps = weights.shape[0]
        operands.append(weights)
        outs.append(jax.ShapeDtypeStruct(weights.shape, F32))
        scratch += [
            pltpu.VMEM(weights.shape, F32),
            pltpu.SemaphoreType.DMA((comps,)),
            pltpu.SemaphoreType.DMA((comps,)),
        ]
    return pl.pallas_call(
        functools.partial(relax_kernel, count, comps),
        out_shape=outs,
        in_specs=[pl.BlockSpec(memory_space=pltpu.SMEM)] + [vmem] * (len(operands) - 1),
        out_specs=[vmem] * len(outs),
        scratch_shapes=scratch,
        compiler_params=pltpu.CompilerParams(
            collective_id=0 if comps else 1, has_side_effects=True, vmem_limit_bytes=VMEM_LIMIT
        ),
        name="relax",
    )(*operands)


def gather_kernel(strides, live_ref, state_ref, base_ref, weight_ref, out_ref, packed):
    nvar, pairs, width_z = state_ref.shape
    width_y, shift = strides
    tiles, _, tile = base_ref.shape
    for v in range(nvar):
        high, low = split(state_ref[v])
        packed[v * pairs : (v + 1) * pairs, :width_z] = high
        packed[v * pairs : (v + 1) * pairs, width_z:] = low

    def one(t, carry):
        @pl.when(live_ref[t] > 0)
        def _():
            base = base_ref[t]
            pair = lax.shift_right_logical(base, shift)
            depth = jnp.bitwise_and(base, width_z - 1)
            depth = jnp.concatenate([depth, depth + 1], axis=1)
            pair = jnp.concatenate([pair, pair], axis=1)
            at_z = lax.broadcasted_iota(jnp.int32, (width_z, 2 * tile), 0)
            hot = jnp.where(at_z == depth, 1.0, 0.0).astype(BF16)
            hot = jnp.concatenate([hot, hot], axis=0)
            found = jnp.dot(packed[...], hot, preferred_element_type=F32)
            at_pair = lax.broadcasted_iota(jnp.int32, (pairs, 2 * tile), 0) - pair
            weights = weight_ref[t]
            spread = jnp.zeros((pairs, 2 * tile), F32)
            for i in range(2):
                for j in range(2):
                    k = 4 * i + 2 * j
                    row = jnp.concatenate([weights[k : k + 1], weights[k + 1 : k + 2]], axis=1)
                    spread = jnp.where(at_pair == i * width_y + j, row, spread)
            total = (found.reshape(nvar, pairs, 2 * tile) * spread[None]).sum(axis=1)
            out_ref[t] = total[:, :tile] + total[:, tile:]

        @pl.when(live_ref[t] <= 0)
        def _():
            out_ref[t] = jnp.zeros((nvar, tile), F32)

        return carry

    lax.fori_loop(0, tiles, one, 0)


def gather(live, state, base, weights):
    nvar, rows, width_y, width_z = state.shape
    pairs = rows * width_y
    tiles, _, tile = base.shape
    vmem = pl.BlockSpec(memory_space=pltpu.VMEM)
    return pl.pallas_call(
        functools.partial(gather_kernel, (width_y, width_z.bit_length() - 1)),
        out_shape=jax.ShapeDtypeStruct((tiles, nvar, tile), F32),
        in_specs=[pl.BlockSpec(memory_space=pltpu.SMEM)] + [vmem] * 3,
        out_specs=vmem,
        scratch_shapes=[pltpu.VMEM((nvar * pairs, 2 * width_z), BF16)],
        compiler_params=pltpu.CompilerParams(vmem_limit_bytes=VMEM_LIMIT),
        name="gather",
    )(live, state.reshape(nvar, pairs, width_z), base, weights)


def scatter_kernel(
    comps, shift, state_ref, cell_ref, value_ref, out_ref,
    rows_ref, total, landing, send_sem, recv_sem,
):
    nvar, pairs, width_z = state_ref.shape
    slots, tile = cell_ref.shape[1], cell_ref.shape[3]
    barrier = pltpu.get_barrier_semaphore()
    greet_comps(comps, barrier)
    mine, copy = comp_copies(comps, value_ref, landing, send_sem, recv_sem)
    pl.semaphore_wait(barrier, comps - 1)
    for d in range(1, comps):
        copy(d).start()
    landing[0] = value_ref[mine]
    for s in range(slots):
        low_at = slice((2 * s + 1) * tile, (2 * s + 2) * tile)
        rows_ref[nvar * pairs :, low_at] = jnp.zeros((pairs, tile), BF16)

    def one(d, carry):
        @pl.when(d > 0)
        def _():
            copy(d).wait_recv()

        source = lax.rem(mine - d + comps, comps)
        hots = []
        for s in range(slots):
            cell = cell_ref[source, s]
            pair = lax.shift_right_arithmetic(cell, shift)
            depth = jnp.bitwise_and(cell, width_z - 1)
            hot = lax.broadcasted_iota(jnp.int32, (width_z, tile), 0) == depth
            hot = jnp.where(hot, 1.0, 0.0).astype(BF16)
            hots += [hot, hot]
            here = lax.broadcasted_iota(jnp.int32, (pairs, tile), 0) == pair
            values = landing[d, s]
            high = values.astype(BF16).astype(F32)
            low = values - high
            high_at = slice(2 * s * tile, (2 * s + 1) * tile)
            low_at = slice((2 * s + 1) * tile, (2 * s + 2) * tile)
            for v in range(nvar):
                at = slice(v * pairs, (v + 1) * pairs)
                rows_ref[at, high_at] = jnp.where(here, high[v : v + 1], 0.0).astype(BF16)
                rows_ref[at, low_at] = jnp.where(here, low[v : v + 1], 0.0).astype(BF16)
            rows_ref[nvar * pairs :, high_at] = jnp.where(here, 1.0, 0.0).astype(BF16)
        part = lax.dot_general(
            rows_ref[...], jnp.concatenate(hots, axis=1), (((1,), (1,)), ((), ())),
            preferred_element_type=F32,
        )

        @pl.when(d == 0)
        def _():
            total[...] = part

        @pl.when(d > 0)
        def _():
            total[...] += part

        return carry

    lax.fori_loop(0, comps, one, 0)
    hit = total[nvar * pairs :, :] > 0.5
    for v in range(nvar):
        out_ref[v] = jnp.where(hit, total[v * pairs : (v + 1) * pairs, :], state_ref[v])
    for d in range(1, comps):
        copy(d).wait_send()


def scatter(state, cells, values):
    nvar, rows, width_y, width_z = state.shape
    pairs = rows * width_y
    comps, slots, _, tile = cells.shape
    vmem = pl.BlockSpec(memory_space=pltpu.VMEM)
    out = pl.pallas_call(
        functools.partial(scatter_kernel, comps, width_z.bit_length() - 1),
        out_shape=jax.ShapeDtypeStruct((nvar, pairs, width_z), F32),
        in_specs=[vmem] * 3,
        out_specs=vmem,
        scratch_shapes=[
            pltpu.VMEM(((nvar + 1) * pairs, 2 * slots * tile), BF16),
            pltpu.VMEM(((nvar + 1) * pairs, width_z), F32),
            pltpu.VMEM(values.shape, F32),
            pltpu.SemaphoreType.DMA((comps,)),
            pltpu.SemaphoreType.DMA((comps,)),
        ],
        compiler_params=pltpu.CompilerParams(
            collective_id=2, has_side_effects=True, vmem_limit_bytes=VMEM_LIMIT
        ),
        name="scatter",
    )(state.reshape(nvar, pairs, width_z), cells, values)
    return out.reshape(state.shape)


def shards(
    state_now, state_prev, viscosity, jacobian, donor_cell, interp_weight, recv_cell, pair_tiles
):
    now = state_now[0]
    prev = state_prev[0]
    kappa = viscosity[0]
    jac = jacobian[0]
    nvar = now.shape[0]
    comps = lax.axis_size("comp")
    mine = lax.axis_index("comp")
    slots, corners, tile = donor_cell.shape[3:]
    tiles = comps * slots
    slot = jnp.arange(slots, dtype=jnp.int32)[None, :]
    live_in = lax.dynamic_index_in_dim(pair_tiles[0], mine, 1, keepdims=False)
    live_out = lax.dynamic_index_in_dim(pair_tiles[0], mine, 0, keepdims=False)
    keep = (slot < live_in[:, None]).reshape(comps, slots, 1, 1)
    cells = jnp.where(keep, recv_cell[0, 0].reshape(comps, slots, 1, tile), -1)
    send = (slot < live_out[:, None]).astype(jnp.int32).reshape(tiles)
    base = donor_cell[0, 0].reshape(tiles, corners, tile)[:, :1]
    state, held = relax(jac, now, now, prev, kappa, interp_weight[0, 0])
    held = held.reshape(tiles, corners, tile)
    for sub in range(SUBITERS):
        if sub > 0:
            (state,) = relax(jac, state, now, prev, kappa)
        packed = gather(send, state, base, held)
        state = scatter(state, cells, packed.reshape(comps, slots, nvar, tile))
    return state[None]


def solution(mesh):
    in_specs = (
        P("comp", None, "blk", None, None),
        P("comp", None, "blk", None, None),
        P("comp", "blk", None, None),
        P("comp", None, None, None),
        P("comp", "blk", None, None, None, None),
        P("comp", "blk", None, None, None, None),
        P("comp", "blk", None, None, None),
        P("blk", None, None),
    )
    out_specs = P("comp", None, "blk", None, None)
    return jax.shard_map(shards, mesh=mesh, in_specs=in_specs, out_specs=out_specs, check_vma=False)
```
